32 devices in a mesh: row: 8 (over z, core), col: 4 (over y, x).
Axes of the slice: x: 2, y: 2, z: 4, core: 2. Of those that a mesh axis runs over, the one named last changes fastest.
Arguments:
- local_inverse: float32 [256, 512, 512], P(('row', 'col')), may hold values from -1 to 3.5, as said below
- coupling: float32 [256, 512, 1024], P(('row', 'col')), may hold values from -0.0625 to 0.0625
- local_rhs: float32 [256, 512], P(('row', 'col')), may hold values from -6 to 6
- members: int32 [256, 8], P(('row', 'col')), may hold values from 0 to 15, all different within a row
- shared_matrix: float32 [2048, 2048], P('row', 'col'), may hold values from -2 to 66, as said below
- shared_rhs: float32 [2048], P('row'), may hold values from -6 to 6
- prior_solution: float32 [2048], P('row'), may hold values from -6 to 6
- preconditioner: float32 [2048], P('row'), may hold values from 0.008 to 0.02
Outputs:
- reduced_matrix: float32 [2048, 2048], P('row', 'col')
- reduced_rhs: float32 [2048], P('row')
- solution: float32 [2048], P('row')
The draws below stay inside these ranges and needn't reach their ends.
Inputs may be any that keep to these rules, and one draw needn't show every extreme that they name: `members`: each week names 8 different station blocks. `local_inverse`: symmetric for every week. `shared_matrix`: symmetric.
All inputs are finite; a program needn't handle non-finite values.
Results may differ from the reference program's by a relative error of at most 0.00016.
Values sent between devices are 32-bit elements; how exact they have to be, the bound alone decides.
A program may use at most 256 MiB of HBM per device.

```python
import math
import jax
import jax.numpy as jnp
from jax import lax

LOCAL = 512
BLOCK = 128
BLOCKS = 16
TOUCHED = 8
ITERS = 2
WEEKS = 256
SHARED = 2048


def draw_local_inverse(key, part):
    first, second = jax.random.split(jax.random.fold_in(key, 11))
    diagonal = jax.random.uniform(first, (WEEKS, LOCAL), jnp.float32, 1.0, 2.0)
    noise = jax.random.truncated_normal(second, -4.0, 4.0, (WEEKS, LOCAL, LOCAL), jnp.float32)
    spread = 0.4 / math.sqrt(2.0 * LOCAL)
    symmetric = (noise + jnp.swapaxes(noise, 1, 2)) * spread
    return symmetric + diagonal[:, :, None] * jnp.eye(LOCAL, dtype=jnp.float32)[None, :, :]


def draw_shared_matrix(key, part):
    first, second = jax.random.split(jax.random.fold_in(key, 23))
    diagonal = jax.random.uniform(first, (SHARED,), jnp.float32, 45.0, 60.0)
    noise = jax.random.truncated_normal(second, -4.0, 4.0, (SHARED, SHARED), jnp.float32)
    spread = 2.2 / math.sqrt(2.0 * SHARED)
    symmetric = (noise + noise.T) * spread
    return symmetric + jnp.diag(diagonal)


def levels(stream_key, shape, cuts, least, largest):
    level, own = 1.0, jax.random.fold_in(stream_key, 6)
    for dim, shards_of in cuts:
        heights = jnp.exp(jax.random.uniform(jax.random.fold_in(own, dim), (shards_of,), jnp.float32, least / len(cuts), largest / len(cuts)))
        level = level * jnp.repeat(heights, shape[dim] // shards_of).reshape([-1 if axis == dim else 1 for axis in range(len(shape))])
    return level


def different_ones(stream_key, rows, amount, top, lift):
    sequence = jax.random.permutation(jax.random.fold_in(stream_key, 1), amount)
    pull = sequence
    for power in range(3):
        pull = pull * pull // amount
    pull = pull * lift // amount
    tickets = jax.random.randint(jax.random.fold_in(stream_key, 2), (rows, amount), 0, 4096) + pull
    sure = jax.random.permutation(jax.random.fold_in(stream_key, 3), rows)[jnp.arange(amount) % rows]
    tickets = jnp.where(jnp.arange(rows)[:, None] == sure[None, :], 1 << 14, tickets)
    priority = tickets * amount + jnp.arange(amount)
    return lax.top_k(priority.astype(jnp.int32), top)[1].astype(jnp.int32)


def centred(stream_key, shape, scale, most, shards=(), held_as=jnp.bfloat16):
    entries = scale * jax.random.normal(stream_key, shape, jnp.float32)
    if shards:
        entries = entries * levels(stream_key, shape, shards, -0.22, 0.18)
    return jnp.clip(entries, -most, most).astype(held_as)


def setup_inputs(seed: int = 0) -> dict:
    keys = jax.random.split(jax.random.key(seed), 9)
    return {
        "local_inverse": draw_local_inverse(jax.random.fold_in(keys[8], 71), 0),
        "coupling": centred(keys[1], (WEEKS, LOCAL, TOUCHED * BLOCK), (LOCAL * WEEKS // 16) ** -0.5, 0.0625, ((0, 32),), jnp.float32),
        "local_rhs": centred(keys[2], (WEEKS, LOCAL), 1.0, 6.0, ((0, 32),), jnp.float32),
        "members": different_ones(keys[3], WEEKS, BLOCKS, TOUCHED, 4096),
        "shared_matrix": draw_shared_matrix(jax.random.fold_in(keys[8], 71), 0),
        "shared_rhs": centred(keys[5], (SHARED,), 1.0, 6.0, ((0, 8),), jnp.float32),
        "prior_solution": centred(keys[6], (SHARED,), 1.0, 6.0, ((0, 8),), jnp.float32),
        "preconditioner": jnp.clip(jnp.exp(math.log(0.02) - 0.91629066 * jax.random.uniform(keys[7], (SHARED,), jnp.float32) ** levels(keys[7], (SHARED,), ((0, 8),), -0.2, 0.2)), 0.008, 0.02),
    }


def eliminate(accumulated, items):
    grid_sum, rhs_sum = accumulated
    inverse, coupling_week, rhs_week, blocks = items
    mapped = jnp.dot(inverse, coupling_week, precision=lax.Precision.HIGHEST, preferred_element_type=jnp.float32)
    contribution = jnp.dot(coupling_week.T, mapped, precision=lax.Precision.HIGHEST, preferred_element_type=jnp.float32)
    pushed = jnp.dot(rhs_week, mapped, precision=lax.Precision.HIGHEST, preferred_element_type=jnp.float32)
    tile_grid = contribution.reshape(TOUCHED, BLOCK, TOUCHED, BLOCK).transpose(0, 2, 1, 3)
    grid_sum = grid_sum.at[blocks[:, None], blocks[None, :]].add(tile_grid)
    rhs_sum = rhs_sum.at[blocks].add(pushed.reshape(TOUCHED, BLOCK))
    return (grid_sum, rhs_sum), None


def reference(local_inverse, coupling, local_rhs, members, shared_matrix, shared_rhs, prior_solution, preconditioner):
    start_grid = jnp.zeros((BLOCKS, BLOCKS, BLOCK, BLOCK), jnp.float32)
    start_rhs = jnp.zeros((BLOCKS, BLOCK), jnp.float32)
    (grid_sum, rhs_sum), unused = lax.scan(eliminate, (start_grid, start_rhs), (local_inverse, coupling, local_rhs, members.astype(jnp.int32)))
    eliminated = grid_sum.transpose(0, 2, 1, 3).reshape(SHARED, SHARED)
    reduced_matrix = shared_matrix - eliminated
    reduced_rhs = shared_rhs - rhs_sum.reshape(SHARED)
    solution = prior_solution
    for iteration in range(ITERS):
        product = jnp.dot(reduced_matrix, solution, precision=lax.Precision.HIGHEST, preferred_element_type=jnp.float32)
        solution = solution + preconditioner * (reduced_rhs - product)
    return (reduced_matrix, reduced_rhs, solution)
```

```python
import functools
import math

import jax
import jax.numpy as jnp
from jax import lax
from jax.experimental import pallas as pl
from jax.experimental.pallas import tpu as pltpu
from jax.sharding import PartitionSpec as P

ITERS = 2
CHUNKS = 9
LEAD = 16
MESH = pl.DeviceIdType.MESH


def halves(value):
    high = value.astype(jnp.bfloat16)
    return high, (value - high.astype(jnp.float32)).astype(jnp.bfloat16)


def axis_bits(row_count, column_count):
    row_bits = [1 << i for i in range(row_count.bit_length() - 1)]
    column_bits = [1 << i for i in range(column_count.bit_length() - 1)]
    axes = [("row", row_bits[0])]
    axes += [("col", bit) for bit in column_bits]
    axes += [("row", bit) for bit in row_bits[1:]]
    return axes


def arrivals(orders, sizes, axes):
    count, free, events = len(axes), {}, []
    pending = [(0.0, 0, chunk) for chunk in range(len(orders))]
    while pending:
        pending.sort()
        ready, level, chunk = pending.pop(0)
        axis = orders[chunk][level]
        name, bit = axes[axis]
        link = "core" if axis == 0 else "long" if name == "row" else axis
        volume = sizes[chunk] * (1 << (count - 1 - level)) / 544 / 16
        spent = volume * (7.0 if axis == 0 else 48.0) * (bit // 2 if link == "long" else 1)
        begin = max(ready, free.get(link, 0.0))
        free[link] = begin + spent
        events.append((begin + spent + 2.0, level, chunk))
        if level + 1 < count:
            pending.append((begin + spent + 2.0, level + 1, chunk))
    return [(level, chunk) for landing, level, chunk in sorted(events)]


def eliminate_kernel(
    touched, block, blocks, row_blocks, week_count,
    members_ref, inverse_ref, coupling_ref, rhs_ref, total, rhs_out, *scratch,
):
    operands = (scratch[0:3], scratch[3:6])
    stacked, rhs_total, order, member = scratch[6:]
    turn = pl.program_id(0)
    weeks = pl.num_programs(0) - 1
    size = inverse_ref.shape[1]
    step = 2
    groups = touched // step
    newest = jnp.minimum(turn, weeks - 1)

    @pl.when(turn == 0)
    def _():
        total[...] = jnp.zeros_like(total)
        rhs_total[...] = jnp.zeros_like(rhs_total)
        rhs_out[...] = jnp.zeros_like(rhs_out)

        def rank_week(week, carry):
            names = [members_ref[week, k] for k in range(touched)]
            for k, name in enumerate(names):
                rank = sum((other < name).astype(jnp.int32) for other in names)
                order[week, rank] = k
                member[week, rank] = name
            return carry

        lax.fori_loop(0, week_count, rank_week, 0)

    def prepare(buffers, group):
        left, right, flipped = buffers
        rows = slice(group * size // groups, (group + 1) * size // groups)
        high, low = halves(inverse_ref[0, rows, :])
        left[rows, 0:size] = high
        left[rows, size : 2 * size] = low
        if group == 0:
            high, low = halves(jnp.broadcast_to(rhs_ref[pl.ds(newest, 1), :], (LEAD, size)))
            flipped[0:LEAD, 0:size] = high
            flipped[0:LEAD, size : 2 * size] = low
        for k in range(group * step, (group + 1) * step):
            at = pl.multiple_of(order[newest, k] * block, block)
            part = coupling_ref[0, :, pl.ds(at, block)]
            columns = slice(k * block, (k + 1) * block)
            high, low = halves(part)
            right[0:size, columns] = high
            right[size : 2 * size, columns] = low
            high, low = halves(part.T)
            rows = slice(LEAD + k * block, LEAD + (k + 1) * block)
            flipped[rows, 0:size] = high
            flipped[rows, size : 2 * size] = low

    def three_term(first, rows, second, columns):
        high, low = first[rows, 0:size], first[rows, size : 2 * size]
        top, bottom = second[0:size, columns], second[size : 2 * size, columns]
        return jnp.dot(
            jnp.concatenate([high, high, low], axis=1),
            jnp.concatenate([top, bottom, top], axis=0),
            preferred_element_type=jnp.float32,
        )

    def map_group(buffers, j):
        left, right, flipped = buffers
        columns = slice(j * step * block, (j + 1) * step * block)
        mapped = three_term(left, slice(0, size), right, columns)
        high, low = halves(mapped)
        stacked[0:size, columns] = high
        stacked[size : 2 * size, columns] = low

    def multiply(buffers, j, places, bases):
        left, right, flipped = buffers
        columns = slice(j * step * block, (j + 1) * step * block)
        rows = LEAD + (j + 1) * step * block
        product = three_term(flipped, slice(0, rows), stacked, columns)
        for half in range(step):
            l = j * step + half
            lanes = slice(half * block, (half + 1) * block)
            rhs_total[places[l]] += product[0:8, lanes]
            for k in range(l + 1):
                at = pl.ds(pl.multiple_of((bases[k] + places[l]) * block, block), block)
                total[at, :] += product[LEAD + k * block : LEAD + (k + 1) * block, lanes]

    def run(new, old):
        if old is not None:
            places = [member[turn - 1, k] for k in range(touched)]
            bases = [
                jnp.where(a < blocks // 2, a * blocks, (blocks - 1 - a) * (blocks + 1) + 1)
                for a in places
            ]
            for group in range(groups):
                map_group(operands[old], group)
        for group in range(groups):
            if new is not None:
                prepare(operands[new], group)
            if old is not None:
                multiply(operands[old], group, places, bases)

    middle = jnp.logical_and(turn > 0, turn < weeks)
    odd = lax.rem(turn, 2) == 1
    pl.when(turn == 0)(lambda: run(0, None))
    pl.when(jnp.logical_and(middle, odd))(lambda: run(1, 0))
    pl.when(jnp.logical_and(middle, jnp.logical_not(odd)))(lambda: run(0, 1))
    pl.when(turn == weeks)(lambda: run(None, (week_count - 1) % 2))

    @pl.when(turn == weeks)
    def _():
        for b in range(blocks):
            owner, place = b // row_blocks, b % row_blocks
            rhs_out[owner, place : place + 1, :] = rhs_total[b, 0:1, :]


def combine_kernel(
    block, blocks, axes, section_rows, row_count, column_count,
    packed, parts, shared, rhs, prior, scale,
    tile, rhs_out, solution_out, *scratch,
):
    count = len(axes)
    landed = scratch[:count]
    (
        xs, across, downs, sums, vsource, vbuf,
        step_send, step_recv, piece_send, tile_sem,
        x_send, x_recv, v_send, v_recv,
    ) = scratch[count:]
    r, c = lax.axis_index("row"), lax.axis_index("col")
    row_blocks, column_blocks = blocks // row_count, blocks // column_count
    piece = math.gcd(section_rows, block)

    def bit_of(i):
        name, bit = axes[i]
        return lax.rem((r if name == "row" else c) // bit, 2)

    bits = [bit_of(i) for i in range(count)]

    def partner(i):
        name, bit = axes[i]
        move = bit * (1 - 2 * bits[i])
        return (r + move, c) if name == "row" else (r, c + move)

    def over_rows(body):
        def each(offset, carry):
            body(offset, lax.rem(r + offset, row_count))
            return carry

        lax.fori_loop(1, row_count, each, 0)

    def over_columns(body):
        for offset in range(1, column_count):
            body(offset, lax.rem(c + offset, column_count))

    def x_copy(k, offset, other):
        own = pl.ds(r * row_blocks, row_blocks)
        return pltpu.make_async_remote_copy(
            src_ref=xs.at[k, own],
            dst_ref=xs.at[k, own],
            send_sem=x_send.at[k, offset - 1],
            recv_sem=x_recv.at[k, r],
            device_id=(other, c),
            device_id_type=MESH,
        )

    def await_x(k, offset, other):
        theirs = xs.at[k, pl.ds(other * row_blocks, row_blocks)]
        pltpu.make_async_copy(theirs, theirs, x_recv.at[k, other]).wait()

    def over_all(body):
        def each(offset, carry):
            body(
                offset,
                lax.rem(r + offset // column_count, row_count),
                lax.rem(c + offset, column_count),
            )
            return carry

        lax.fori_loop(1, row_count * column_count, each, 0)

    def v_copy(k, offset, row, column):
        return pltpu.make_async_remote_copy(
            src_ref=vsource.at[k, row],
            dst_ref=vbuf.at[k, r * column_count + c],
            send_sem=v_send.at[k, offset - 1],
            recv_sem=v_recv.at[k, r * column_count + c],
            device_id=(row, column),
            device_id_type=MESH,
        )

    def rows_of(value):
        return jnp.concatenate(
            [value[i : i + 1, :] for i in range(value.shape[0])], axis=1
        )

    def publish(k, current):
        for i in range(row_blocks):
            xs[k, r * row_blocks + i] = jnp.broadcast_to(
                current[:, i * block : (i + 1) * block], xs.shape[2:]
            )
        over_rows(lambda offset, other: x_copy(k, offset, other).start())

    def multiply(k):
        over_rows(lambda offset, other: await_x(k, offset, other))
        across[...] = jnp.zeros_like(across)
        tall = block // 8

        lead = (blocks // 2).bit_length() - 1

        def stored(p, o):
            parts = []
            for row in range(o * block, (o + 1) * block, piece):
                s, offset = divmod(row, section_rows)
                spot = tuple(lax.rem(p >> (lead - 1 - i), 2) for i in range(lead))
                spot += tuple((s >> (count - lead - 1 - i)) & 1 for i in range(count - lead))
                parts.append(packed[spot + (pl.ds(offset, piece),)])
            return jnp.concatenate(parts, axis=0).reshape(tall, 8, block)

        def by_pair(p, carry):
            ends = (p, blocks - 1 - p)
            for side in range(2):
                row = jnp.broadcast_to(xs[k, ends[side], 0:1, :], (block, block))
                downs[side] = row.T.reshape(tall, 8, block)
                sums[side] = jnp.zeros_like(sums[side])
            for o in range(blocks + 1):
                upper = o < blocks - p
                side = 0 if o <= blocks // 2 else 1 if o == blocks else jnp.where(upper, 0, 1)
                b = jnp.where(upper, p + o, o - 1)
                keep = jnp.where(b == jnp.where(upper, ends[0], ends[1]), 0.0, 1.0)
                part = stored(p, o)
                across[b] += jnp.sum(part * downs[side], axis=0) * keep
                sums[side] += part * xs[k, b][None]
            for side in range(2):
                flat = sums[side].reshape(block, block).T
                across[ends[side]] += jnp.sum(flat.reshape(tall, 8, block), axis=0)
            return carry

        lax.fori_loop(0, blocks // 2, by_pair, 0)
        for b in range(blocks):
            owner, place = b // row_blocks, row_blocks + b % row_blocks
            vsource[k, owner, place : place + 1, :] = jnp.sum(
                across[b], axis=0, keepdims=True
            )
        for i in range(row_blocks):
            along = jnp.zeros((tall, 8, block), jnp.float32)
            for j in range(column_blocks):
                part = shared[i * block : (i + 1) * block, j * block : (j + 1) * block]
                along = along + part.reshape(tall, 8, block) * xs[k, c * column_blocks + j][None]
            flat = jnp.sum(along.reshape(block, block).T, axis=0, keepdims=True)
            place = slice(row_blocks + i, row_blocks + i + 1)
            vsource[k, r, place, :] = vsource[k, r, place, :] - flat
        vbuf[k, r * column_count + c] = vsource[k, r]
        over_all(lambda *where: v_copy(k, *where).start())

    def update(k, current):
        def arrive(offset, row, column):
            source = row * column_count + column
            pltpu.make_async_copy(
                vsource.at[k, row], vbuf.at[k, source], v_recv.at[k, source]
            ).wait()

        over_all(arrive)
        summed = vbuf[k, 0]
        for i in range(1, row_count * column_count):
            summed = summed + vbuf[k, i]
        if k == 0:
            rhs_out[...] = rhs[...] - rows_of(summed[0:row_blocks])
        return current + scale[...] * (
            rhs_out[...] + rows_of(summed[row_blocks : 2 * row_blocks])
        )

    pieces, per_block = section_rows // piece, block // piece
    cuts = [pieces * i // CHUNKS for i in range(CHUNKS + 1)]
    edges = [piece * cut for cut in cuts]
    low = [i for i in range(count) if axes[i][0] == "col"]
    rest = [i for i in range(1, count) if axes[i][0] == "row"]
    kinds = [
        [0] + rest[:1] + low + rest[1:],
        [0] + low + rest,
        [0] + low[::-1] + rest,
        [0] + rest[:1] + low[::-1] + rest[1:],
        [0] + low + rest,
        [0] + low[::-1] + rest,
    ]
    orders = [kinds[chunk % len(kinds)] for chunk in range(CHUNKS)]

    def half(chunk, level, own):
        done = orders[chunk][:level]
        left_axes = [i for i in range(count) if i not in done]
        axis = orders[chunk][level]
        at = left_axes.index(axis)
        pick = bits[axis] if own else 1 - bits[axis]
        rows = pl.ds(edges[chunk], edges[chunk + 1] - edges[chunk])
        return (
            (slice(None),) * at + (pick,) + (slice(None),) * (len(left_axes) - at - 1) + (rows,)
        )

    def exchange(chunk, level):
        source = packed if level == 0 else landed[level - 1]
        rows = pl.ds(edges[chunk], edges[chunk + 1] - edges[chunk])
        target = (slice(None),) * (count - level - 1) + (rows,)
        return pltpu.make_async_remote_copy(
            src_ref=source.at[half(chunk, level, False)],
            dst_ref=landed[level].at[target],
            send_sem=step_send.at[level, chunk],
            recv_sem=step_recv.at[level, chunk],
            device_id=partner(orders[chunk][level]),
            device_id_type=MESH,
        )

    def greet():
        barrier = pltpu.get_barrier_semaphore()

        def signal(row, column):
            pl.semaphore_signal(
                barrier, inc=1, device_id=(row, column), device_id_type=MESH
            )

        over_rows(lambda offset, other: signal(other, c))
        over_columns(lambda offset, other: signal(r, other))
        pl.semaphore_wait(barrier, row_count + column_count - 2)

    greet()
    for chunk in range(CHUNKS):
        exchange(chunk, 0).start()
    publish(0, prior[...])
    final = landed[count - 1]
    section = sum(bits[i] * (1 << (count - 1 - i)) for i in range(count))

    def piece_plan(q):
        g = section * pieces + q
        t, part = g // per_block, lax.rem(g, per_block)
        p, o = t // (blocks + 1), lax.rem(t, blocks + 1)
        upper = o < blocks - p
        a = jnp.where(upper, p, blocks - 1 - p)
        b = jnp.where(upper, p + o, o - 1)
        plans = []
        for which, (i, j) in enumerate(((a, b), (b, a))):
            dr, dc = i // row_blocks, j // column_blocks
            own = jnp.logical_and(dr == r, dc == c)
            live = True if which == 0 else a != b
            source = final.at[pl.ds(pl.multiple_of(q * piece, piece), piece)]
            target = tile.at[
                lax.rem(i, row_blocks),
                lax.rem(j, column_blocks),
                pl.ds(pl.multiple_of(part * piece, piece), piece),
            ]
            remote = pltpu.make_async_remote_copy(
                src_ref=source,
                dst_ref=target,
                send_sem=piece_send.at[which, q],
                recv_sem=tile_sem,
                device_id=(dr, dc),
                device_id_type=MESH,
            )
            local = pltpu.make_async_copy(source, target, tile_sem)
            plans.append((jnp.logical_and(live, own), local, jnp.logical_and(live, jnp.logical_not(own)), remote))
        return plans

    def send_piece(q, carry):
        for near, local, far, remote in piece_plan(q):
            pl.when(near)(local.start)
            pl.when(far)(remote.start)
        return carry

    def finish_piece(q, carry):
        for near, local, far, remote in piece_plan(q):
            pl.when(far)(remote.wait_send)
        return carry

    sizes = [edges[i + 1] - edges[i] for i in range(CHUNKS)]
    events = arrivals(orders, sizes, axes)
    last = [
        max(i for i, event in enumerate(events) if event[0] == level) for level in range(count)
    ]
    current = None

    def stage(number):
        nonlocal current
        k = number // 2
        if number == 0:
            current = prior[...]
            vsource[0] = parts[...]
            for later in range(1, ITERS):
                vsource[later] = jnp.zeros_like(vsource[later])
        if number % 2 == 0:
            multiply(k)
        else:
            current = update(k, current)
            if k + 1 < ITERS:
                publish(k + 1, current)
            else:
                solution_out[...] = current

    stages = {last[min(i, count - 1)] + max(0, i + 1 - count): i for i in range(2 * ITERS)}
    for index, (level, chunk) in enumerate(events):
        exchange(chunk, level).wait_recv()
        rows = pl.ds(edges[chunk], sizes[chunk])
        target = (slice(None),) * (count - level - 1) + (rows,)
        before = packed if level == 0 else landed[level - 1]
        landed[level][target] = landed[level][target] + before[half(chunk, level, True)]
        if level + 1 < count:
            exchange(chunk, level + 1).start()
        else:
            lax.fori_loop(cuts[chunk], cuts[chunk + 1], send_piece, 0)
        if index in stages:
            stage(stages[index])
    pltpu.make_async_copy(tile, tile, tile_sem).wait()
    for k in range(ITERS):
        over_rows(lambda offset, other: x_copy(k, offset, other).wait_send())
        over_all(lambda *where: v_copy(k, *where).wait_send())
    for level in range(count):
        for chunk in range(CHUNKS):
            exchange(chunk, level).wait_send()
    lax.fori_loop(0, pieces, finish_piece, 0)


def finish_kernel(
    block, row_blocks, column_blocks,
    tile, shared_ref, rhs_ref, current_ref, matrix_out, rhs_out, solution_out,
):
    r, c = lax.axis_index("row"), lax.axis_index("col")
    for i in range(row_blocks):
        for j in range(column_blocks):
            at = (slice(i * block, (i + 1) * block), slice(j * block, (j + 1) * block))
            part = tile[i, j]
            straight = r * row_blocks + i <= c * column_blocks + j
            matrix_out[at] = shared_ref[at] - jnp.where(straight, part, part.T)
    rhs_out[...] = rhs_ref[...]
    solution_out[...] = current_ref[...]


def local(
    local_inverse,
    coupling,
    local_rhs,
    members,
    shared_matrix,
    shared_rhs,
    prior_solution,
    preconditioner,
):
    row_count = lax.axis_size("row")
    column_count = lax.axis_size("col")
    weeks, size, wide = coupling.shape
    touched = members.shape[1]
    block = wide // touched
    blocks = shared_matrix.shape[0] * row_count // block
    row_blocks = blocks // row_count
    tile_rows, tile_columns = shared_matrix.shape
    axes = axis_bits(row_count, column_count)
    count = len(axes)
    sections = 1 << count
    flat_rows = blocks * (blocks + 1) // 2 * block
    section_rows = flat_rows // sections
    extra = -(-2 * row_blocks // 8) * 8
    f32, bf16 = jnp.float32, jnp.bfloat16

    packed, parts = pl.pallas_call(
        functools.partial(
            eliminate_kernel, touched, block, blocks, row_blocks, weeks
        ),
        grid_spec=pltpu.PrefetchScalarGridSpec(
            num_scalar_prefetch=1,
            grid=(weeks + 1,),
            in_specs=[pl.BlockSpec((1, size, size), lambda w, m: (jnp.minimum(w, weeks - 1), 0, 0))]
            + [pl.BlockSpec((1, size, wide), lambda w, m: (jnp.minimum(w, weeks - 1), 0, 0))]
            + [pl.BlockSpec((weeks, size), lambda w, m: (0, 0))],
            out_specs=[pl.BlockSpec(memory_space=pltpu.VMEM)] * 2,
            scratch_shapes=[
                *[
                    pltpu.VMEM((size, 2 * size), bf16),
                    pltpu.VMEM((2 * size, wide), bf16),
                    pltpu.VMEM((LEAD + wide, 2 * size), bf16),
                ]
                * 2,
                pltpu.VMEM((2 * size, wide), bf16),
                pltpu.VMEM((blocks, 8, block), f32),
                pltpu.SMEM((weeks, touched), jnp.int32),
                pltpu.SMEM((weeks, touched), jnp.int32),
            ],
        ),
        out_shape=[
            pltpu.VMEM((flat_rows, block), f32),
            pltpu.VMEM((row_count, extra, block), f32),
        ],
        compiler_params=pltpu.CompilerParams(dimension_semantics=("arbitrary",), vmem_limit_bytes=52 << 20),
        name="eliminate",
    )(members, local_inverse, coupling, local_rhs)

    vmem = pl.BlockSpec(memory_space=pltpu.VMEM)
    dma = pltpu.SemaphoreType.DMA
    pieces = section_rows // math.gcd(section_rows, block)
    row = (1, tile_rows)
    column_blocks = blocks // column_count
    tile, reduced_rhs, updated = pl.pallas_call(
        functools.partial(
            combine_kernel, block, blocks, axes, section_rows, row_count, column_count
        ),
        in_specs=[vmem] * 6,
        out_specs=[vmem] * 3,
        out_shape=[
            jax.ShapeDtypeStruct((row_blocks, column_blocks, block, block), f32),
            jax.ShapeDtypeStruct(row, f32),
            jax.ShapeDtypeStruct(row, f32),
        ],
        scratch_shapes=[
            pltpu.VMEM((2,) * (count - level - 1) + (section_rows, block), f32)
            for level in range(count)
        ]
        + [
            pltpu.VMEM((ITERS, blocks, 8, block), f32),
            pltpu.VMEM((blocks, 8, block), f32),
            pltpu.VMEM((2, block // 8, 8, block), f32),
            pltpu.VMEM((2, block // 8, 8, block), f32),
            pltpu.VMEM((ITERS, row_count, extra, block), f32),
            pltpu.VMEM((ITERS, sections, extra, block), f32),
            dma((count, CHUNKS)),
            dma((count, CHUNKS)),
            dma((2, pieces)),
            dma,
            dma((ITERS, row_count - 1)),
            dma((ITERS, row_count)),
            dma((ITERS, sections - 1)),
            dma((ITERS, sections)),
        ],
        compiler_params=pltpu.CompilerParams(has_side_effects=True, collective_id=0, vmem_limit_bytes=32 << 20),
        name="combine",
    )(
        packed.reshape((2,) * count + (section_rows, block)),
        parts,
        shared_matrix,
        shared_rhs.reshape(row),
        prior_solution.reshape(row),
        preconditioner.reshape(row),
    )
    reduced_matrix, reduced_rhs, updated = pl.pallas_call(
        functools.partial(finish_kernel, block, row_blocks, column_blocks),
        in_specs=[vmem] * 4,
        out_specs=[vmem] * 3,
        out_shape=[
            jax.ShapeDtypeStruct((tile_rows, tile_columns), f32),
            jax.ShapeDtypeStruct(row, f32),
            jax.ShapeDtypeStruct(row, f32),
        ],
        compiler_params=pltpu.CompilerParams(vmem_limit_bytes=8 << 20),
        name="finish",
    )(tile, shared_matrix, reduced_rhs, updated)
    return reduced_matrix, reduced_rhs.reshape(tile_rows), updated.reshape(tile_rows)


def solution(mesh):
    return jax.shard_map(
        local,
        mesh=mesh,
        in_specs=(
            P(("row", "col"), None, None),
            P(("row", "col"), None, None),
            P(("row", "col"), None),
            P(("row", "col"), None),
            P("row", "col"),
            P("row"),
            P("row"),
            P("row"),
        ),
        out_specs=(P("row", "col"), P("row"), P("row")),
        check_vma=False,
    )
```

```python
import functools
import math

import jax
import jax.numpy as jnp
from jax import lax
from jax.experimental import pallas as pl
from jax.experimental.pallas import tpu as pltpu
from jax.sharding import PartitionSpec as P

ITERS = 2
CHUNKS = 9
SPLIT = 8
LEAD = 16
MESH = pl.DeviceIdType.MESH


def halves(value):
    high = value.astype(jnp.bfloat16)
    return high, (value - high.astype(jnp.float32)).astype(jnp.bfloat16)


def axis_bits(row_count, column_count):
    row_bits = [1 << i for i in range(row_count.bit_length() - 1)]
    column_bits = [1 << i for i in range(column_count.bit_length() - 1)]
    axes = [("row", row_bits[0])]
    axes += [("col", bit) for bit in column_bits]
    axes += [("row", bit) for bit in row_bits[1:]]
    return axes


def arrivals(orders, sizes, axes):
    count, free, events = len(axes), {}, []
    pending = [(0.0, 0, chunk) for chunk in range(len(orders))]
    while pending:
        pending.sort()
        ready, level, chunk = pending.pop(0)
        axis = orders[chunk][level]
        name, bit = axes[axis]
        link = "core" if axis == 0 else "long" if name == "row" else axis
        volume = sizes[chunk] * (1 << (count - 1 - level)) / 544 / 16
        spent = volume * (7.0 if axis == 0 else 48.0) * (bit // 2 if link == "long" else 1)
        begin = max(ready, free.get(link, 0.0))
        free[link] = begin + spent
        events.append((begin + spent + 2.0, level, chunk))
        if level + 1 < count:
            pending.append((begin + spent + 2.0, level + 1, chunk))
    return [(level, chunk) for landing, level, chunk in sorted(events)]


def eliminate_kernel(
    touched, block, blocks, row_blocks, week_count,
    members_ref, inverse_ref, coupling_ref, rhs_ref, total, rhs_out, *scratch,
):
    operands = (scratch[0:3], scratch[3:6])
    stacked, rhs_total, order, member = scratch[6:]
    turn = pl.program_id(0)
    weeks = pl.num_programs(0) - 1
    size = inverse_ref.shape[1]
    step = 2
    groups = touched // step
    newest = jnp.minimum(turn, weeks - 1)

    def clear():
        total[...] = jnp.zeros_like(total)
        rhs_total[...] = jnp.zeros_like(rhs_total)
        rhs_out[...] = jnp.zeros_like(rhs_out)

    def rank_week():
        names = [members_ref[newest, k] for k in range(touched)]
        for k, name in enumerate(names):
            rank = sum((other < name).astype(jnp.int32) for other in names)
            order[newest, rank] = k
            member[newest, rank] = name

    def prepare(buffers, group):
        left, right, flipped = buffers
        rows = slice(group * size // groups, (group + 1) * size // groups)
        high, low = halves(inverse_ref[0, rows, :])
        left[rows, 0:size] = high
        left[rows, size : 2 * size] = low
        if group == 0:
            high, low = halves(jnp.broadcast_to(rhs_ref[pl.ds(newest, 1), :], (LEAD, size)))
            flipped[0:LEAD, 0:size] = high
            flipped[0:LEAD, size : 2 * size] = low
        for k in range(group * step, (group + 1) * step):
            at = pl.multiple_of(order[newest, k] * block, block)
            part = coupling_ref[0, :, pl.ds(at, block)]
            columns = slice(k * block, (k + 1) * block)
            high, low = halves(part)
            right[0:size, columns] = high
            right[size : 2 * size, columns] = low
            high, low = halves(part.T)
            rows = slice(LEAD + k * block, LEAD + (k + 1) * block)
            flipped[rows, 0:size] = high
            flipped[rows, size : 2 * size] = low

    def three_term(first, rows, second, columns):
        high, low = first[rows, 0:size], first[rows, size : 2 * size]
        top, bottom = second[0:size, columns], second[size : 2 * size, columns]
        return jnp.dot(
            jnp.concatenate([high, high, low], axis=1),
            jnp.concatenate([top, bottom, top], axis=0),
            preferred_element_type=jnp.float32,
        )

    def map_group(buffers, j):
        left, right, flipped = buffers
        columns = slice(j * step * block, (j + 1) * step * block)
        mapped = three_term(left, slice(0, size), right, columns)
        high, low = halves(mapped)
        stacked[0:size, columns] = high
        stacked[size : 2 * size, columns] = low

    def multiply(buffers, j, places, bases):
        left, right, flipped = buffers
        columns = slice(j * step * block, (j + 1) * step * block)
        rows = LEAD + (j + 1) * step * block
        product = three_term(flipped, slice(0, rows), stacked, columns)
        for half in range(step):
            l = j * step + half
            lanes = slice(half * block, (half + 1) * block)
            rhs_total[places[l]] += product[0:8, lanes]
            for k in range(l + 1):
                at = pl.ds(pl.multiple_of((bases[k] + places[l]) * block, block), block)
                total[at, :] += product[LEAD + k * block : LEAD + (k + 1) * block, lanes]

    def run(new, old):
        if new is not None:
            rank_week()
        if old is None:
            clear()
        if old is not None:
            places = [member[turn - 1, k] for k in range(touched)]
            bases = [
                jnp.where(a < blocks // 2, a * blocks, (blocks - 1 - a) * (blocks + 1) + 1)
                for a in places
            ]
            for group in range(groups):
                map_group(operands[old], group)
        for group in range(groups):
            if new is not None:
                prepare(operands[new], group)
            if old is not None:
                multiply(operands[old], group, places, bases)

    middle = jnp.logical_and(turn > 0, turn < weeks)
    odd = lax.rem(turn, 2) == 1
    pl.when(turn == 0)(lambda: run(0, None))
    pl.when(jnp.logical_and(middle, odd))(lambda: run(1, 0))
    pl.when(jnp.logical_and(middle, jnp.logical_not(odd)))(lambda: run(0, 1))
    pl.when(turn == weeks)(lambda: run(None, (week_count - 1) % 2))

    @pl.when(turn == weeks)
    def _():
        for b in range(blocks):
            owner, place = b // row_blocks, b % row_blocks
            rhs_out[owner, place : place + 1, :] = rhs_total[b, 0:1, :]


def combine_kernel(
    block, blocks, axes, section_rows, row_count, column_count,
    packed, parts, shared, rhs, prior, scale,
    tile, rhs_out, solution_out, *scratch,
):
    count = len(axes)
    landed = scratch[:count]
    (
        xs, across, downs, sums, vsource, vbuf,
        step_send, step_recv, piece_send, tile_sem,
        x_send, x_recv, v_send, v_recv,
    ) = scratch[count:]
    r, c = lax.axis_index("row"), lax.axis_index("col")
    row_blocks, column_blocks = blocks // row_count, blocks // column_count
    piece = math.gcd(section_rows, block)

    def bit_of(i):
        name, bit = axes[i]
        return lax.rem((r if name == "row" else c) // bit, 2)

    bits = [bit_of(i) for i in range(count)]

    def partner(i):
        name, bit = axes[i]
        move = bit * (1 - 2 * bits[i])
        return (r + move, c) if name == "row" else (r, c + move)

    def over_rows(body):
        for i in range(1, row_count):
            body((r + i) & (row_count - 1))

    def over_columns(body):
        for j in range(1, column_count):
            body((c + j) & (column_count - 1))

    def x_copy(k, other):
        own = pl.ds(r * row_blocks, row_blocks)
        return pltpu.make_async_remote_copy(
            src_ref=xs.at[k, own],
            dst_ref=xs.at[k, own],
            send_sem=x_send.at[k],
            recv_sem=x_recv.at[k],
            device_id=(other, c),
            device_id_type=MESH,
        )

    def settle(region, sem):
        pltpu.make_async_copy(region, region, sem).wait()

    def settle_x(k, sems):
        settle(xs.at[k, pl.ds(0, blocks - row_blocks)], sems.at[k])

    def settle_v(k, sems):
        settle(vbuf.at[k, pl.ds(0, row_count * column_count - 1)], sems.at[k])

    def over_all(body):
        def each(i, carry):
            for j in range(column_count):
                body((r + i) & (row_count - 1), (c + j) & (column_count - 1))
            return carry

        for j in range(1, column_count):
            body(r, (c + j) & (column_count - 1))
        lax.fori_loop(1, row_count, each, 0)

    def v_copy(k, row, column):
        return pltpu.make_async_remote_copy(
            src_ref=vsource.at[k, row],
            dst_ref=vbuf.at[k, r * column_count + c],
            send_sem=v_send.at[k],
            recv_sem=v_recv.at[k],
            device_id=(row, column),
            device_id_type=MESH,
        )

    def rows_of(value):
        return jnp.concatenate(
            [value[i : i + 1, :] for i in range(value.shape[0])], axis=1
        )

    def publish(k, current):
        for i in range(row_blocks):
            xs[k, r * row_blocks + i] = jnp.broadcast_to(
                current[:, i * block : (i + 1) * block], xs.shape[2:]
            )
        over_rows(lambda other: x_copy(k, other).start())

    tall = block // 8
    lead = (blocks // 2).bit_length() - 1

    def multiply(k, begin, end):
        if begin == 0:
            settle_x(k, x_recv)
            across[...] = jnp.zeros_like(across)

        def stored(p, o):
            parts = []
            for row in range(o * block, (o + 1) * block, piece):
                s, offset = divmod(row, section_rows)
                spot = tuple(lax.rem(p >> (lead - 1 - i), 2) for i in range(lead))
                spot += tuple((s >> (count - lead - 1 - i)) & 1 for i in range(count - lead))
                parts.append(packed[spot + (pl.ds(offset, piece),)])
            return jnp.concatenate(parts, axis=0).reshape(tall, 8, block)

        def by_pair(p, carry):
            ends = (p, blocks - 1 - p)
            for side in range(2):
                row = jnp.broadcast_to(xs[k, ends[side], 0:1, :], (block, block))
                downs[side] = row.T.reshape(tall, 8, block)
            along = jnp.zeros((tall, 8, block), jnp.float32)
            for o in range(blocks + 1):
                upper = o < blocks - p
                side = 0 if o <= blocks // 2 else 1 if o == blocks else jnp.where(upper, 0, 1)
                b = jnp.where(upper, p + o, o - 1)
                keep = jnp.where(b == jnp.where(upper, ends[0], ends[1]), 0.0, 1.0)
                part = stored(p, o)
                across[b] += jnp.sum(part * downs[side], axis=0) * keep
                if o <= blocks // 2:
                    along = along + part * xs[k, b][None]
                    if o == blocks // 2:
                        sums[0] = along
                        sums[1] = jnp.zeros_like(along)
                else:
                    sums[side] += part * xs[k, b][None]
            for side in range(2):
                flat = sums[side].reshape(block, block).T
                across[ends[side]] += jnp.sum(flat.reshape(tall, 8, block), axis=0)
            return carry

        lax.fori_loop(begin, end, by_pair, 0)
        if end < blocks // 2:
            return
        for b in range(blocks):
            owner, place = b // row_blocks, row_blocks + b % row_blocks
            vsource[k, owner, place : place + 1, :] = jnp.sum(
                across[b], axis=0, keepdims=True
            )
        for i in range(row_blocks):
            along = jnp.zeros((tall, 8, block), jnp.float32)
            for j in range(column_blocks):
                part = shared[i * block : (i + 1) * block, j * block : (j + 1) * block]
                along = along + part.reshape(tall, 8, block) * xs[k, c * column_blocks + j][None]
            flat = jnp.sum(along.reshape(block, block).T, axis=0, keepdims=True)
            place = slice(row_blocks + i, row_blocks + i + 1)
            vsource[k, r, place, :] = vsource[k, r, place, :] - flat
        vbuf[k, r * column_count + c] = vsource[k, r]
        over_all(lambda row, column: v_copy(k, row, column).start())

    def update(k, current):
        settle_v(k, v_recv)
        summed = vbuf[k, 0]
        for i in range(1, row_count * column_count):
            summed = summed + vbuf[k, i]
        if k == 0:
            rhs_out[...] = rhs[...] - rows_of(summed[0:row_blocks])
        return current + scale[...] * (
            rhs_out[...] + rows_of(summed[row_blocks : 2 * row_blocks])
        )

    pieces, per_block = section_rows // piece, block // piece
    cuts = [pieces * i // CHUNKS for i in range(CHUNKS + 1)]
    edges = [piece * cut for cut in cuts]
    low = [i for i in range(count) if axes[i][0] == "col"]
    rest = [i for i in range(1, count) if axes[i][0] == "row"]
    kinds = [
        [0] + rest[:1] + low + rest[1:],
        [0] + low + rest,
        [0] + low[::-1] + rest,
        [0] + rest[:1] + low[::-1] + rest[1:],
        [0] + low + rest,
        [0] + low[::-1] + rest,
    ]
    orders = [kinds[chunk % len(kinds)] for chunk in range(CHUNKS)]

    def half(chunk, level, own):
        done = orders[chunk][:level]
        left_axes = [i for i in range(count) if i not in done]
        axis = orders[chunk][level]
        at = left_axes.index(axis)
        pick = bits[axis] if own else 1 - bits[axis]
        rows = pl.ds(edges[chunk], edges[chunk + 1] - edges[chunk])
        return (
            (slice(None),) * at + (pick,) + (slice(None),) * (len(left_axes) - at - 1) + (rows,)
        )

    def exchange(chunk, level):
        source = packed if level == 0 else landed[level - 1]
        rows = pl.ds(edges[chunk], edges[chunk + 1] - edges[chunk])
        target = (slice(None),) * (count - level - 1) + (rows,)
        return pltpu.make_async_remote_copy(
            src_ref=source.at[half(chunk, level, False)],
            dst_ref=landed[level].at[target],
            send_sem=step_send.at[level],
            recv_sem=step_recv.at[level, chunk],
            device_id=partner(orders[chunk][level]),
            device_id_type=MESH,
        )

    def greet():
        barrier = pltpu.get_barrier_semaphore()

        def signal(row, column):
            pl.semaphore_signal(
                barrier, inc=1, device_id=(row, column), device_id_type=MESH
            )

        over_rows(lambda other: signal(other, c))
        over_columns(lambda other: signal(r, other))
        pl.semaphore_wait(barrier, row_count + column_count - 2)

    greet()
    for chunk in range(CHUNKS):
        exchange(chunk, 0).start()
    publish(0, prior[...])
    final = landed[count - 1]
    section = sum(bits[i] * (1 << (count - 1 - i)) for i in range(count))

    def quotient(value, by):
        factor = -(-(1 << 16) // by)
        whole = (value * factor) >> 16
        return whole, value - whole * by

    def piece_plan(q):
        g = section * pieces + q
        t, part = quotient(g, per_block)
        p, o = quotient(t, blocks + 1)
        upper = o < blocks - p
        a = jnp.where(upper, p, blocks - 1 - p)
        b = jnp.where(upper, p + o, o - 1)
        plans = []
        for which, (i, j) in enumerate(((a, b), (b, a))):
            dr, i = quotient(i, row_blocks)
            dc, j = quotient(j, column_blocks)
            own = jnp.logical_and(dr == r, dc == c)
            live = True if which == 0 else a != b
            source = final.at[pl.ds(pl.multiple_of(q * piece, piece), piece)]
            target = tile.at[
                i, j, pl.ds(pl.multiple_of(part * piece, piece), piece),
            ]
            remote = pltpu.make_async_remote_copy(
                src_ref=source,
                dst_ref=target,
                send_sem=piece_send.at[which, q],
                recv_sem=tile_sem,
                device_id=(dr, dc),
                device_id_type=MESH,
            )
            local = pltpu.make_async_copy(source, target, tile_sem)
            plans.append((jnp.logical_and(live, own), local, jnp.logical_and(live, jnp.logical_not(own)), remote))
        return plans

    def send_piece(q, carry):
        for near, local, far, remote in piece_plan(q):
            pl.when(near)(local.start)
            pl.when(far)(remote.start)
        return carry

    def finish_piece(q, carry):
        for near, local, far, remote in piece_plan(q):
            pl.when(far)(remote.wait_send)
        return carry

    sizes = [edges[i + 1] - edges[i] for i in range(CHUNKS)]
    events = arrivals(orders, sizes, axes)
    last = [
        max(i for i, event in enumerate(events) if event[0] == level) for level in range(count)
    ]
    current = None

    pairs = blocks // 2

    def stage(k, begin, end):
        nonlocal current
        if k == 0 and begin == 0:
            current = prior[...]
            vsource[0] = parts[...]
            for later in range(1, ITERS):
                vsource[later] = jnp.zeros_like(vsource[later])
        if begin < pairs:
            multiply(k, begin, end)
            return
        current = update(k, current)
        if k + 1 < ITERS:
            publish(k + 1, current)
        else:
            solution_out[...] = current

    stages = {last[0]: (0, 0, pairs), last[1]: (0, pairs, pairs)}
    start = min(last[2], len(events) - SPLIT)
    for i in range(SPLIT):
        stages[start + i] = (1, i * pairs // SPLIT, (i + 1) * pairs // SPLIT)
    for index, (level, chunk) in enumerate(events):
        exchange(chunk, level).wait_recv()
        rows = pl.ds(edges[chunk], sizes[chunk])
        target = (slice(None),) * (count - level - 1) + (rows,)
        before = packed if level == 0 else landed[level - 1]
        landed[level][target] = landed[level][target] + before[half(chunk, level, True)]
        if level + 1 < count:
            exchange(chunk, level + 1).start()
        else:
            lax.fori_loop(cuts[chunk], cuts[chunk + 1], send_piece, 0)
        if index in stages:
            stage(*stages[index])
    for level in range(count):
        settle(landed[level], step_send.at[level])
    for k in range(ITERS):
        settle_x(k, x_send)
        settle_v(k, v_send)
    stage(ITERS - 1, pairs, pairs)
    lax.fori_loop(0, pieces, finish_piece, 0)
    pltpu.make_async_copy(tile, tile, tile_sem).wait()


def finish_kernel(
    block, row_blocks, column_blocks,
    tile, shared_ref, rhs_ref, current_ref, matrix_out, rhs_out, solution_out,
):
    r, c = lax.axis_index("row"), lax.axis_index("col")
    for i in range(row_blocks):
        for j in range(column_blocks):
            at = (slice(i * block, (i + 1) * block), slice(j * block, (j + 1) * block))
            part = tile[i, j]
            straight = r * row_blocks + i <= c * column_blocks + j
            matrix_out[at] = shared_ref[at] - jnp.where(straight, part, part.T)
    rhs_out[...] = rhs_ref[...]
    solution_out[...] = current_ref[...]


def local(
    local_inverse,
    coupling,
    local_rhs,
    members,
    shared_matrix,
    shared_rhs,
    prior_solution,
    preconditioner,
):
    row_count = lax.axis_size("row")
    column_count = lax.axis_size("col")
    weeks, size, wide = coupling.shape
    touched = members.shape[1]
    block = wide // touched
    blocks = shared_matrix.shape[0] * row_count // block
    row_blocks = blocks // row_count
    tile_rows, tile_columns = shared_matrix.shape
    axes = axis_bits(row_count, column_count)
    count = len(axes)
    sections = 1 << count
    flat_rows = blocks * (blocks + 1) // 2 * block
    section_rows = flat_rows // sections
    extra = -(-2 * row_blocks // 8) * 8
    f32, bf16 = jnp.float32, jnp.bfloat16

    packed, parts = pl.pallas_call(
        functools.partial(
            eliminate_kernel, touched, block, blocks, row_blocks, weeks
        ),
        grid_spec=pltpu.PrefetchScalarGridSpec(
            num_scalar_prefetch=1,
            grid=(weeks + 1,),
            in_specs=[pl.BlockSpec((1, size, size), lambda w, m: (jnp.minimum(w, weeks - 1), 0, 0))]
            + [pl.BlockSpec((1, size, wide), lambda w, m: (jnp.minimum(w, weeks - 1), 0, 0))]
            + [pl.BlockSpec((weeks, size), lambda w, m: (0, 0))],
            out_specs=[pl.BlockSpec(memory_space=pltpu.VMEM)] * 2,
            scratch_shapes=[
                *[
                    pltpu.VMEM((size, 2 * size), bf16),
                    pltpu.VMEM((2 * size, wide), bf16),
                    pltpu.VMEM((LEAD + wide, 2 * size), bf16),
                ]
                * 2,
                pltpu.VMEM((2 * size, wide), bf16),
                pltpu.VMEM((blocks, 8, block), f32),
                pltpu.SMEM((weeks, touched), jnp.int32),
                pltpu.SMEM((weeks, touched), jnp.int32),
            ],
        ),
        out_shape=[
            pltpu.VMEM((flat_rows, block), f32),
            pltpu.VMEM((row_count, extra, block), f32),
        ],
        compiler_params=pltpu.CompilerParams(dimension_semantics=("arbitrary",), vmem_limit_bytes=52 << 20),
        name="eliminate",
    )(members, local_inverse, coupling, local_rhs)

    vmem = pl.BlockSpec(memory_space=pltpu.VMEM)
    dma = pltpu.SemaphoreType.DMA
    pieces = section_rows // math.gcd(section_rows, block)
    row = (1, tile_rows)
    column_blocks = blocks // column_count
    tile, reduced_rhs, updated = pl.pallas_call(
        functools.partial(
            combine_kernel, block, blocks, axes, section_rows, row_count, column_count
        ),
        in_specs=[vmem] * 6,
        out_specs=[vmem] * 3,
        out_shape=[
            jax.ShapeDtypeStruct((row_blocks, column_blocks, block, block), f32),
            jax.ShapeDtypeStruct(row, f32),
            jax.ShapeDtypeStruct(row, f32),
        ],
        scratch_shapes=[
            pltpu.VMEM((2,) * (count - level - 1) + (section_rows, block), f32)
            for level in range(count)
        ]
        + [
            pltpu.VMEM((ITERS, blocks, 8, block), f32),
            pltpu.VMEM((blocks, 8, block), f32),
            pltpu.VMEM((2, block // 8, 8, block), f32),
            pltpu.VMEM((2, block // 8, 8, block), f32),
            pltpu.VMEM((ITERS, row_count, extra, block), f32),
            pltpu.VMEM((ITERS, sections, extra, block), f32),
            dma((count,)),
            dma((count, CHUNKS)),
            dma((2, pieces)),
            dma,
            dma((ITERS,)),
            dma((ITERS,)),
            dma((ITERS,)),
            dma((ITERS,)),
        ],
        compiler_params=pltpu.CompilerParams(has_side_effects=True, collective_id=0, vmem_limit_bytes=32 << 20),
        name="combine",
    )(
        packed.reshape((2,) * count + (section_rows, block)),
        parts,
        shared_matrix,
        shared_rhs.reshape(row),
        prior_solution.reshape(row),
        preconditioner.reshape(row),
    )
    reduced_matrix, reduced_rhs, updated = pl.pallas_call(
        functools.partial(finish_kernel, block, row_blocks, column_blocks),
        in_specs=[vmem] * 4,
        out_specs=[vmem] * 3,
        out_shape=[
            jax.ShapeDtypeStruct((tile_rows, tile_columns), f32),
            jax.ShapeDtypeStruct(row, f32),
            jax.ShapeDtypeStruct(row, f32),
        ],
        compiler_params=pltpu.CompilerParams(vmem_limit_bytes=8 << 20),
        name="finish",
    )(tile, shared_matrix, reduced_rhs, updated)
    return reduced_matrix, reduced_rhs.reshape(tile_rows), updated.reshape(tile_rows)


def solution(mesh):
    return jax.shard_map(
        local,
        mesh=mesh,
        in_specs=(
            P(("row", "col"), None, None),
            P(("row", "col"), None, None),
            P(("row", "col"), None),
            P(("row", "col"), None),
            P("row", "col"),
            P("row"),
            P("row"),
            P("row"),
        ),
        out_specs=(P("row", "col"), P("row"), P("row")),
        check_vma=False,
    )
```

```python
import functools
import math

import jax
import jax.numpy as jnp
from jax import lax
from jax.experimental import pallas as pl
from jax.experimental.pallas import tpu as pltpu
from jax.sharding import PartitionSpec as P

ITERS = 2
CHUNKS = 9
SPLIT = 8
LEAD = 16
MESH = pl.DeviceIdType.MESH


def halves(value):
    high = value.astype(jnp.bfloat16)
    return high, (value - high.astype(jnp.float32)).astype(jnp.bfloat16)


def axis_bits(row_count, column_count):
    row_bits = [1 << i for i in range(row_count.bit_length() - 1)]
    column_bits = [1 << i for i in range(column_count.bit_length() - 1)]
    axes = [("row", row_bits[0])]
    axes += [("col", bit) for bit in column_bits]
    axes += [("row", bit) for bit in row_bits[:0:-1]]
    return axes


def arrivals(orders, sizes, axes):
    count, free, events = len(axes), {}, []
    pending = [(0.0, 0, chunk) for chunk in range(len(orders))]
    while pending:
        pending.sort()
        ready, level, chunk = pending.pop(0)
        axis = orders[chunk][level]
        name, bit = axes[axis]
        link = "core" if axis == 0 else "long" if name == "row" else axis
        volume = sizes[chunk] * (1 << (count - 1 - level)) / 544 / 16
        spent = volume * (7.0 if axis == 0 else 48.0) * (bit // 2 if link == "long" else 1)
        begin = max(ready, free.get(link, 0.0))
        free[link] = begin + spent
        events.append((begin + spent + 2.0, level, chunk))
        if level + 1 < count:
            pending.append((begin + spent + 2.0, level + 1, chunk))
    return [(level, chunk) for landing, level, chunk in sorted(events)]


def eliminate_kernel(
    touched, block, blocks, row_blocks, week_count,
    members_ref, inverse_ref, coupling_ref, rhs_ref, total, rhs_out, *scratch,
):
    operands = (scratch[0:3], scratch[3:6])
    stacked, rhs_total, order, member = scratch[6:]
    turn = pl.program_id(0)
    weeks = pl.num_programs(0) - 1
    size = inverse_ref.shape[1]
    step = 2
    groups = touched // step
    newest = jnp.minimum(turn, weeks - 1)

    def clear():
        total[...] = jnp.zeros_like(total)
        rhs_total[...] = jnp.zeros_like(rhs_total)
        rhs_out[...] = jnp.zeros_like(rhs_out)

    def rank_week():
        names = [members_ref[newest, k] for k in range(touched)]
        for k, name in enumerate(names):
            rank = sum((other < name).astype(jnp.int32) for other in names)
            order[newest, rank] = k
            member[newest, rank] = name

    def prepare(buffers, group):
        left, right, flipped = buffers
        rows = slice(group * size // groups, (group + 1) * size // groups)
        high, low = halves(inverse_ref[0, rows, :])
        left[rows, 0:size] = high
        left[rows, size : 2 * size] = low
        if group == 0:
            high, low = halves(jnp.broadcast_to(rhs_ref[pl.ds(newest, 1), :], (LEAD, size)))
            flipped[0:LEAD, 0:size] = high
            flipped[0:LEAD, size : 2 * size] = low
        for k in range(group * step, (group + 1) * step):
            at = pl.multiple_of(order[newest, k] * block, block)
            part = coupling_ref[0, :, pl.ds(at, block)]
            columns = slice(k * block, (k + 1) * block)
            high, low = halves(part)
            right[0:size, columns] = high
            right[size : 2 * size, columns] = low
            high, low = halves(part.T)
            rows = slice(LEAD + k * block, LEAD + (k + 1) * block)
            flipped[rows, 0:size] = high
            flipped[rows, size : 2 * size] = low

    def three_term(first, rows, second, columns):
        high, low = first[rows, 0:size], first[rows, size : 2 * size]
        top, bottom = second[0:size, columns], second[size : 2 * size, columns]
        return jnp.dot(
            jnp.concatenate([high, high, low], axis=1),
            jnp.concatenate([top, bottom, top], axis=0),
            preferred_element_type=jnp.float32,
        )

    def map_group(buffers, j):
        left, right, flipped = buffers
        columns = slice(j * step * block, (j + 1) * step * block)
        mapped = three_term(left, slice(0, size), right, columns)
        high, low = halves(mapped)
        stacked[0:size, columns] = high
        stacked[size : 2 * size, columns] = low

    def multiply(buffers, j, places, bases):
        left, right, flipped = buffers
        columns = slice(j * step * block, (j + 1) * step * block)
        rows = LEAD + (j + 1) * step * block
        product = three_term(flipped, slice(0, rows), stacked, columns)
        for half in range(step):
            l = j * step + half
            lanes = slice(half * block, (half + 1) * block)
            rhs_total[places[l]] += product[0:8, lanes]
            for k in range(l + 1):
                at = pl.ds(pl.multiple_of((bases[k] + places[l]) * block, block), block)
                total[at, :] += product[LEAD + k * block : LEAD + (k + 1) * block, lanes]

    def run(new, old):
        if new is not None:
            rank_week()
        if old is None:
            clear()
        if old is not None:
            places = [member[turn - 1, k] for k in range(touched)]
            bases = [
                jnp.where(a < blocks // 2, a * blocks, (blocks - 1 - a) * (blocks + 1) + 1)
                for a in places
            ]
            for group in range(groups):
                map_group(operands[old], group)
        for group in range(groups):
            if new is not None:
                prepare(operands[new], group)
            if old is not None:
                multiply(operands[old], group, places, bases)

    middle = jnp.logical_and(turn > 0, turn < weeks)
    odd = lax.rem(turn, 2) == 1
    pl.when(turn == 0)(lambda: run(0, None))
    pl.when(jnp.logical_and(middle, odd))(lambda: run(1, 0))
    pl.when(jnp.logical_and(middle, jnp.logical_not(odd)))(lambda: run(0, 1))
    pl.when(turn == weeks)(lambda: run(None, (week_count - 1) % 2))

    @pl.when(turn == weeks)
    def _():
        for b in range(blocks):
            owner, place = b // row_blocks, b % row_blocks
            rhs_out[owner, place : place + 1, :] = rhs_total[b, 0:1, :]


def combine_kernel(
    block, blocks, axes, section_rows, row_count, column_count,
    packed, parts, shared, rhs, prior, scale,
    tile, rhs_out, solution_out, *scratch,
):
    count = len(axes)
    landed = scratch[:count]
    (
        xs, across, downs, sums, vsource, vbuf,
        step_send, step_recv, piece_send, tile_sem,
        x_send, x_recv, v_send, v_recv,
    ) = scratch[count:]
    r, c = lax.axis_index("row"), lax.axis_index("col")
    row_blocks, column_blocks = blocks // row_count, blocks // column_count
    piece = math.gcd(section_rows, block)

    def bit_of(i):
        name, bit = axes[i]
        return lax.rem((r if name == "row" else c) // bit, 2)

    bits = [bit_of(i) for i in range(count)]

    def partner(i):
        name, bit = axes[i]
        move = bit * (1 - 2 * bits[i])
        return (r + move, c) if name == "row" else (r, c + move)

    def over_rows(body):
        for i in range(1, row_count):
            body((r + i) & (row_count - 1))

    def over_columns(body):
        for j in range(1, column_count):
            body((c + j) & (column_count - 1))

    def x_copy(k, other):
        own = pl.ds(r * row_blocks, row_blocks)
        return pltpu.make_async_remote_copy(
            src_ref=xs.at[k, own],
            dst_ref=xs.at[k, own],
            send_sem=x_send.at[k],
            recv_sem=x_recv.at[k],
            device_id=(other, c),
            device_id_type=MESH,
        )

    def settle(region, sem):
        pltpu.make_async_copy(region, region, sem).wait()

    def settle_x(k, sems):
        settle(xs.at[k, pl.ds(0, blocks - row_blocks)], sems.at[k])

    def settle_v(k, sems):
        settle(vbuf.at[k, pl.ds(0, row_count * column_count - 1)], sems.at[k])

    def over_all(body):
        def each(i, carry):
            for j in range(column_count):
                body((r + i) & (row_count - 1), (c + j) & (column_count - 1))
            return carry

        for j in range(1, column_count):
            body(r, (c + j) & (column_count - 1))
        lax.fori_loop(1, row_count, each, 0)

    def v_copy(k, row, column):
        return pltpu.make_async_remote_copy(
            src_ref=vsource.at[k, row],
            dst_ref=vbuf.at[k, r * column_count + c],
            send_sem=v_send.at[k],
            recv_sem=v_recv.at[k],
            device_id=(row, column),
            device_id_type=MESH,
        )

    def rows_of(value):
        return jnp.concatenate(
            [value[i : i + 1, :] for i in range(value.shape[0])], axis=1
        )

    def publish(k, current):
        for i in range(row_blocks):
            xs[k, r * row_blocks + i] = jnp.broadcast_to(
                current[:, i * block : (i + 1) * block], xs.shape[2:]
            )
        over_rows(lambda other: x_copy(k, other).start())

    tall = block // 8
    lead = (blocks // 2).bit_length() - 1

    def multiply(k, begin, end):
        if begin == 0:
            settle_x(k, x_recv)
            across[...] = jnp.zeros_like(across)

        def stored(p, o):
            parts = []
            for row in range(o * block, (o + 1) * block, piece):
                s, offset = divmod(row, section_rows)
                spot = tuple(lax.rem(p >> (lead - 1 - i), 2) for i in range(lead))
                spot += tuple((s >> (count - lead - 1 - i)) & 1 for i in range(count - lead))
                parts.append(packed[spot + (pl.ds(offset, piece),)])
            return jnp.concatenate(parts, axis=0).reshape(tall, 8, block)

        def by_pair(p, carry):
            ends = (p, blocks - 1 - p)
            for side in range(2):
                row = jnp.broadcast_to(xs[k, ends[side], 0:1, :], (block, block))
                downs[side] = row.T.reshape(tall, 8, block)
            along = jnp.zeros((tall, 8, block), jnp.float32)
            for o in range(blocks + 1):
                upper = o < blocks - p
                side = 0 if o <= blocks // 2 else 1 if o == blocks else jnp.where(upper, 0, 1)
                b = jnp.where(upper, p + o, o - 1)
                keep = jnp.where(b == jnp.where(upper, ends[0], ends[1]), 0.0, 1.0)
                part = stored(p, o)
                across[b] += jnp.sum(part * downs[side], axis=0) * keep
                if o <= blocks // 2:
                    along = along + part * xs[k, b][None]
                    if o == blocks // 2:
                        sums[0] = along
                        sums[1] = jnp.zeros_like(along)
                else:
                    sums[side] += part * xs[k, b][None]
            for side in range(2):
                flat = sums[side].reshape(block, block).T
                across[ends[side]] += jnp.sum(flat.reshape(tall, 8, block), axis=0)
            return carry

        lax.fori_loop(begin, end, by_pair, 0)
        if end < blocks // 2:
            return
        for b in range(blocks):
            owner, place = b // row_blocks, row_blocks + b % row_blocks
            vsource[k, owner, place : place + 1, :] = jnp.sum(
                across[b], axis=0, keepdims=True
            )
        for i in range(row_blocks):
            along = jnp.zeros((tall, 8, block), jnp.float32)
            for j in range(column_blocks):
                part = shared[i * block : (i + 1) * block, j * block : (j + 1) * block]
                along = along + part.reshape(tall, 8, block) * xs[k, c * column_blocks + j][None]
            flat = jnp.sum(along.reshape(block, block).T, axis=0, keepdims=True)
            place = slice(row_blocks + i, row_blocks + i + 1)
            vsource[k, r, place, :] = vsource[k, r, place, :] - flat
        vbuf[k, r * column_count + c] = vsource[k, r]
        over_all(lambda row, column: v_copy(k, row, column).start())

    def update(k, current):
        settle_v(k, v_recv)
        summed = vbuf[k, 0]
        for i in range(1, row_count * column_count):
            summed = summed + vbuf[k, i]
        if k == 0:
            rhs_out[...] = rhs[...] - rows_of(summed[0:row_blocks])
        return current + scale[...] * (
            rhs_out[...] + rows_of(summed[row_blocks : 2 * row_blocks])
        )

    pieces, per_block = section_rows // piece, block // piece
    cuts = [pieces * i // CHUNKS for i in range(CHUNKS + 1)]
    edges = [piece * cut for cut in cuts]
    low = [i for i in range(count) if axes[i][0] == "col"]
    rest = [i for i in range(1, count) if axes[i][0] == "row"][::-1]
    kinds = [
        [0] + rest[:1] + low + rest[1:],
        [0] + low + rest,
        [0] + low[::-1] + rest,
        [0] + rest[:1] + low[::-1] + rest[1:],
        [0] + low + rest,
        [0] + low[::-1] + rest,
    ]
    orders = [kinds[chunk % len(kinds)] for chunk in range(CHUNKS)]

    def half(chunk, level, own):
        done = orders[chunk][:level]
        left_axes = [i for i in range(count) if i not in done]
        axis = orders[chunk][level]
        at = left_axes.index(axis)
        pick = bits[axis] if own else 1 - bits[axis]
        rows = pl.ds(edges[chunk], edges[chunk + 1] - edges[chunk])
        return (
            (slice(None),) * at + (pick,) + (slice(None),) * (len(left_axes) - at - 1) + (rows,)
        )

    def exchange(chunk, level):
        source = packed if level == 0 else landed[level - 1]
        rows = pl.ds(edges[chunk], edges[chunk + 1] - edges[chunk])
        target = (slice(None),) * (count - level - 1) + (rows,)
        return pltpu.make_async_remote_copy(
            src_ref=source.at[half(chunk, level, False)],
            dst_ref=landed[level].at[target],
            send_sem=step_send.at[level],
            recv_sem=step_recv.at[level, chunk],
            device_id=partner(orders[chunk][level]),
            device_id_type=MESH,
        )

    def greet():
        barrier = pltpu.get_barrier_semaphore()

        def signal(row, column):
            pl.semaphore_signal(
                barrier, inc=1, device_id=(row, column), device_id_type=MESH
            )

        over_rows(lambda other: signal(other, c))
        over_columns(lambda other: signal(r, other))
        pl.semaphore_wait(barrier, row_count + column_count - 2)

    greet()
    for chunk in range(CHUNKS):
        exchange(chunk, 0).start()
    publish(0, prior[...])
    final = landed[count - 1]
    section = sum(bits[i] * (1 << (count - 1 - i)) for i in range(count))

    def quotient(value, by):
        factor = -(-(1 << 16) // by)
        whole = (value * factor) >> 16
        return whole, value - whole * by

    def piece_plan(q):
        g = section * pieces + q
        t, part = quotient(g, per_block)
        p, o = quotient(t, blocks + 1)
        upper = o < blocks - p
        a = jnp.where(upper, p, blocks - 1 - p)
        b = jnp.where(upper, p + o, o - 1)
        plans = []
        for which, (i, j) in enumerate(((a, b), (b, a))):
            dr, i = quotient(i, row_blocks)
            dc, j = quotient(j, column_blocks)
            own = jnp.logical_and(dr == r, dc == c)
            live = True if which == 0 else a != b
            source = final.at[pl.ds(pl.multiple_of(q * piece, piece), piece)]
            target = tile.at[
                i, j, pl.ds(pl.multiple_of(part * piece, piece), piece),
            ]
            remote = pltpu.make_async_remote_copy(
                src_ref=source,
                dst_ref=target,
                send_sem=piece_send.at[which, q],
                recv_sem=tile_sem,
                device_id=(dr, dc),
                device_id_type=MESH,
            )
            local = pltpu.make_async_copy(source, target, tile_sem)
            plans.append((jnp.logical_and(live, own), local, jnp.logical_and(live, jnp.logical_not(own)), remote))
        return plans

    def send_piece(q, carry):
        for near, local, far, remote in piece_plan(q):
            pl.when(near)(local.start)
            pl.when(far)(remote.start)
        return carry

    def finish_piece(q, carry):
        for near, local, far, remote in piece_plan(q):
            pl.when(far)(remote.wait_send)
        return carry

    sizes = [edges[i + 1] - edges[i] for i in range(CHUNKS)]
    events = arrivals(orders, sizes, axes)
    last = [
        max(i for i, event in enumerate(events) if event[0] == level) for level in range(count)
    ]
    current = None

    pairs = blocks // 2

    def stage(k, begin, end):
        nonlocal current
        if k == 0 and begin == 0:
            current = prior[...]
            vsource[0] = parts[...]
            for later in range(1, ITERS):
                vsource[later] = jnp.zeros_like(vsource[later])
        if begin < pairs:
            multiply(k, begin, end)
            return
        current = update(k, current)
        if k + 1 < ITERS:
            publish(k + 1, current)
        else:
            solution_out[...] = current

    stages = {last[0]: (0, 0, pairs), last[1]: (0, pairs, pairs)}
    start = min(last[2], len(events) - SPLIT)
    for i in range(SPLIT):
        stages[start + i] = (1, i * pairs // SPLIT, (i + 1) * pairs // SPLIT)
    for index, (level, chunk) in enumerate(events):
        exchange(chunk, level).wait_recv()
        rows = pl.ds(edges[chunk], sizes[chunk])
        target = (slice(None),) * (count - level - 1) + (rows,)
        before = packed if level == 0 else landed[level - 1]
        landed[level][target] = landed[level][target] + before[half(chunk, level, True)]
        if level + 1 < count:
            exchange(chunk, level + 1).start()
        else:
            lax.fori_loop(cuts[chunk], cuts[chunk + 1], send_piece, 0)
        if index in stages:
            stage(*stages[index])
    for level in range(count):
        settle(landed[level], step_send.at[level])
    for k in range(ITERS):
        settle_x(k, x_send)
        settle_v(k, v_send)
    stage(ITERS - 1, pairs, pairs)
    lax.fori_loop(0, pieces, finish_piece, 0)
    pltpu.make_async_copy(tile, tile, tile_sem).wait()


def finish_kernel(
    block, row_blocks, column_blocks,
    tile, shared_ref, rhs_ref, current_ref, matrix_out, rhs_out, solution_out,
):
    r, c = lax.axis_index("row"), lax.axis_index("col")
    for i in range(row_blocks):
        for j in range(column_blocks):
            at = (slice(i * block, (i + 1) * block), slice(j * block, (j + 1) * block))
            part = tile[i, j]
            straight = r * row_blocks + i <= c * column_blocks + j
            matrix_out[at] = shared_ref[at] - jnp.where(straight, part, part.T)
    rhs_out[...] = rhs_ref[...]
    solution_out[...] = current_ref[...]


def local(
    local_inverse,
    coupling,
    local_rhs,
    members,
    shared_matrix,
    shared_rhs,
    prior_solution,
    preconditioner,
):
    row_count = lax.axis_size("row")
    column_count = lax.axis_size("col")
    weeks, size, wide = coupling.shape
    touched = members.shape[1]
    block = wide // touched
    blocks = shared_matrix.shape[0] * row_count // block
    row_blocks = blocks // row_count
    tile_rows, tile_columns = shared_matrix.shape
    axes = axis_bits(row_count, column_count)
    count = len(axes)
    sections = 1 << count
    flat_rows = blocks * (blocks + 1) // 2 * block
    section_rows = flat_rows // sections
    extra = -(-2 * row_blocks // 8) * 8
    f32, bf16 = jnp.float32, jnp.bfloat16

    packed, parts = pl.pallas_call(
        functools.partial(
            eliminate_kernel, touched, block, blocks, row_blocks, weeks
        ),
        grid_spec=pltpu.PrefetchScalarGridSpec(
            num_scalar_prefetch=1,
            grid=(weeks + 1,),
            in_specs=[pl.BlockSpec((1, size, size), lambda w, m: (jnp.minimum(w, weeks - 1), 0, 0))]
            + [pl.BlockSpec((1, size, wide), lambda w, m: (jnp.minimum(w, weeks - 1), 0, 0))]
            + [pl.BlockSpec((weeks, size), lambda w, m: (0, 0))],
            out_specs=[pl.BlockSpec(memory_space=pltpu.VMEM)] * 2,
            scratch_shapes=[
                *[
                    pltpu.VMEM((size, 2 * size), bf16),
                    pltpu.VMEM((2 * size, wide), bf16),
                    pltpu.VMEM((LEAD + wide, 2 * size), bf16),
                ]
                * 2,
                pltpu.VMEM((2 * size, wide), bf16),
                pltpu.VMEM((blocks, 8, block), f32),
                pltpu.SMEM((weeks, touched), jnp.int32),
                pltpu.SMEM((weeks, touched), jnp.int32),
            ],
        ),
        out_shape=[
            pltpu.VMEM((flat_rows, block), f32),
            pltpu.VMEM((row_count, extra, block), f32),
        ],
        compiler_params=pltpu.CompilerParams(dimension_semantics=("arbitrary",), vmem_limit_bytes=52 << 20),
        name="eliminate",
    )(members, local_inverse, coupling, local_rhs)

    vmem = pl.BlockSpec(memory_space=pltpu.VMEM)
    dma = pltpu.SemaphoreType.DMA
    pieces = section_rows // math.gcd(section_rows, block)
    row = (1, tile_rows)
    column_blocks = blocks // column_count
    tile, reduced_rhs, updated = pl.pallas_call(
        functools.partial(
            combine_kernel, block, blocks, axes, section_rows, row_count, column_count
        ),
        in_specs=[vmem] * 6,
        out_specs=[vmem] * 3,
        out_shape=[
            jax.ShapeDtypeStruct((row_blocks, column_blocks, block, block), f32),
            jax.ShapeDtypeStruct(row, f32),
            jax.ShapeDtypeStruct(row, f32),
        ],
        scratch_shapes=[
            pltpu.VMEM((2,) * (count - level - 1) + (section_rows, block), f32)
            for level in range(count)
        ]
        + [
            pltpu.VMEM((ITERS, blocks, 8, block), f32),
            pltpu.VMEM((blocks, 8, block), f32),
            pltpu.VMEM((2, block // 8, 8, block), f32),
            pltpu.VMEM((2, block // 8, 8, block), f32),
            pltpu.VMEM((ITERS, row_count, extra, block), f32),
            pltpu.VMEM((ITERS, sections, extra, block), f32),
            dma((count,)),
            dma((count, CHUNKS)),
            dma((2, pieces)),
            dma,
            dma((ITERS,)),
            dma((ITERS,)),
            dma((ITERS,)),
            dma((ITERS,)),
        ],
        compiler_params=pltpu.CompilerParams(has_side_effects=True, collective_id=0, vmem_limit_bytes=32 << 20),
        name="combine",
    )(
        packed.reshape((2,) * count + (section_rows, block)),
        parts,
        shared_matrix,
        shared_rhs.reshape(row),
        prior_solution.reshape(row),
        preconditioner.reshape(row),
    )
    reduced_matrix, reduced_rhs, updated = pl.pallas_call(
        functools.partial(finish_kernel, block, row_blocks, column_blocks),
        in_specs=[vmem] * 4,
        out_specs=[vmem] * 3,
        out_shape=[
            jax.ShapeDtypeStruct((tile_rows, tile_columns), f32),
            jax.ShapeDtypeStruct(row, f32),
            jax.ShapeDtypeStruct(row, f32),
        ],
        compiler_params=pltpu.CompilerParams(vmem_limit_bytes=8 << 20),
        name="finish",
    )(tile, shared_matrix, reduced_rhs, updated)
    return reduced_matrix, reduced_rhs.reshape(tile_rows), updated.reshape(tile_rows)


def solution(mesh):
    return jax.shard_map(
        local,
        mesh=mesh,
        in_specs=(
            P(("row", "col"), None, None),
            P(("row", "col"), None, None),
            P(("row", "col"), None),
            P(("row", "col"), None),
            P("row", "col"),
            P("row"),
            P("row"),
            P("row"),
        ),
        out_specs=(P("row", "col"), P("row"), P("row")),
        check_vma=False,
    )
```
